32 devices in a mesh: batch: 4 (over y, core), wide: 8 (over z, x).
Axes of the slice: x: 2, y: 2, z: 4, core: 2. Of those that a mesh axis runs over, the one named last changes fastest.
Arguments:
- tokens: bfloat16 [4, 4096, 1024], P('batch', 'wide'), may hold values from -6 to 6
- cotangent: bfloat16 [4, 4096, 1024], P('batch', 'wide'), may hold values from -6 to 6
- doc_starts: int32 [4, 4096], P('batch', 'wide'), may hold values 0 or 1
- state_resets: int32 [4, 8], P('batch', 'wide'), may hold values 0 or 1
- w_query: bfloat16 [1024, 1024], replicated, may hold values from -0.1875 to 0.1875
- w_key: bfloat16 [1024, 1024], replicated, may hold values from -0.1875 to 0.1875
- w_value: bfloat16 [1024, 1024], replicated, may hold values from -0.1875 to 0.1875
- w_out: bfloat16 [1024, 1024], replicated, may hold values from -0.75 to 0.75
- w_state_out: bfloat16 [1024, 1024], replicated, may hold values from -0.75 to 0.75
- w_up: bfloat16 [1024, 4096], replicated, may hold values from -0.1875 to 0.1875
- w_down: bfloat16 [4096, 1024], replicated, may hold values from -0.09375 to 0.09375
- state_query: bfloat16 [512, 1024], replicated, may hold values from -6 to 6
- init_state: float32 [512, 1024], replicated, may hold values from -6 to 6
- gain_attn: float32 [1024], replicated, may hold values from 0.5 to 1.5
- gain_mlp: float32 [1024], replicated, may hold values from 0.5 to 1.5
- gain_state: float32 [1024], replicated, may hold values from 0.5 to 1.5
- state_gate: float32 [1024], replicated, may hold values from 0.6 to 0.998
- bias_table: float32 [8, 32], replicated, may hold values from -5 to 5
Outputs:
- output: bfloat16 [4, 4096, 1024], P('batch', 'wide')
- tokens_grad: bfloat16 [4, 4096, 1024], P('batch', 'wide')
- w_query_grad: float32 [1024, 1024], P('wide')
- w_key_grad: float32 [1024, 1024], P('wide')
- w_value_grad: float32 [1024, 1024], P('wide')
- w_out_grad: float32 [1024, 1024], P('wide')
- w_state_out_grad: float32 [1024, 1024], P('wide')
- w_up_grad: float32 [1024, 4096], P('wide')
- w_down_grad: float32 [4096, 1024], P('wide')
- state_query_grad: float32 [512, 1024], P('wide')
- init_state_grad: float32 [512, 1024], P('wide')
- gain_attn_grad: float32 [1024], replicated
- gain_mlp_grad: float32 [1024], replicated
- gain_state_grad: float32 [1024], replicated
- state_gate_grad: float32 [1024], replicated
- bias_table_grad: float32 [8, 32], replicated
The draws below stay inside these ranges and needn't reach their ends.
All inputs are finite; a program needn't handle non-finite values. No bound on the sum of `doc_starts` or of `state_resets` on one device may be relied on, other than what follows from the above.
Results may differ from the reference program's by a relative error of at most 0.03.
Values may be sent and summed in bfloat16 or wider, within the bound.
A program may use at most 256 MiB of HBM per device.

```python
import math
import jax
import jax.numpy as jnp
import numpy as np
from jax import lax

D = 1024
H = 8
DH = 128
FF = 4096
W = 512
S = 512
NB = 32
MAXDIST = 128
SEQ_WIN = 8
STREAMS = 4
STREAM = 4096
SEQ = 4096
WINDOWS = 8


def with_ends(array, own_key, low, high):
    extent = array.shape
    index_at = [jax.random.randint(jax.random.fold_in(own_key, axis), (), 0, extent[axis]) for axis in range(len(extent))]
    array = array.at[tuple(index_at)].set(low)
    longest = extent.index(max(extent))
    index_at[longest] = (index_at[longest] + 1) % extent[longest]
    return array.at[tuple(index_at)].set(high)


def steps_of(stream_key, extent, pieces, smallest, top_value):
    factor_of = 1.0
    for axis_at, shards_of in pieces:
        steps = jax.random.uniform(jax.random.fold_in(jax.random.fold_in(stream_key, 6), axis_at), (shards_of,), jnp.float32, smallest / len(pieces), top_value / len(pieces))
        factor_of = factor_of * jnp.repeat(jnp.exp(steps), extent[axis_at] // shards_of).reshape((-1,) + (1,) * (len(extent) - 1 - axis_at))
    return factor_of


def scatter_about(own_key, shape, deviation, bound, pieces=(), kind=jnp.bfloat16):
    values = jax.random.normal(own_key, shape, jnp.float32) * deviation
    if len(pieces) > 0:
        values = steps_of(own_key, shape, pieces, -0.22, 0.18) * values
    return jnp.clip(values, min=-bound, max=bound).astype(kind)


def setup_inputs(seed: int = 0) -> dict:
    splits = jax.random.split(jax.random.key(seed), 19)
    return {
        "tokens": scatter_about(splits[0], (STREAMS, STREAM, D), 1.0, 6.0, ((0, 4), (1, 8))),
        "cotangent": scatter_about(splits[1], (STREAMS, STREAM, D), 1.0, 6.0, ((0, 4), (1, 8))),
        "doc_starts": with_ends((jax.random.randint(splits[2], (STREAMS, STREAM), 0, 256) < 1).astype(jnp.int32), jax.random.fold_in(splits[2], 1), 0, 1),
        "state_resets": with_ends((jax.random.randint(splits[3], (STREAMS, WINDOWS), 0, 4) < 1).astype(jnp.int32), jax.random.fold_in(splits[3], 1), 0, 1),
        "w_query": scatter_about(splits[4], (D, D), D ** -0.5, 0.1875),
        "w_key": scatter_about(splits[5], (D, D), D ** -0.5, 0.1875),
        "w_value": scatter_about(splits[6], (D, D), D ** -0.5, 0.1875),
        "w_out": scatter_about(splits[7], (D, D), (D // 16) ** -0.5, 0.75),
        "w_state_out": scatter_about(splits[8], (D, D), (D // 16) ** -0.5, 0.75),
        "w_up": scatter_about(splits[9], (D, FF), D ** -0.5, 0.1875),
        "w_down": scatter_about(splits[10], (FF, D), FF ** -0.5, 0.09375),
        "state_query": scatter_about(splits[11], (S, D), 1.0, 6.0),
        "init_state": scatter_about(splits[12], (S, D), 1.0, 6.0, (), jnp.float32),
        "gain_attn": jnp.clip(1.0 + 0.1 * jax.random.normal(splits[13], (D,), jnp.float32), 0.5, 1.5),
        "gain_mlp": jnp.clip(1.0 + 0.1 * jax.random.normal(splits[14], (D,), jnp.float32), 0.5, 1.5),
        "gain_state": jnp.clip(1.0 + 0.1 * jax.random.normal(splits[15], (D,), jnp.float32), 0.5, 1.5),
        "state_gate": jnp.clip(jax.random.uniform(splits[16], (D,), jnp.float32, 0.6, 0.998), 0.6, 0.998),
        "bias_table": scatter_about(splits[17], (H, NB), 1.0, 5.0, (), jnp.float32),
    }


@jax.custom_vjp
def low(v):
    return lax.optimization_barrier(v.astype(jnp.bfloat16)).astype(jnp.float32)

@jax.custom_vjp
def low_back(v):
    return v

def low_keep(v):
    return (low(v), None)

def low_pass(kept, grad):
    return (grad,)

def back_keep(v):
    return (v, None)

def back_low(kept, grad):
    return (low(grad),)
low.defvjp(low_keep, low_pass)
low_back.defvjp(back_keep, back_low)
epsilon = 1e-06
highest = lax.Precision.HIGHEST

def bucket_onehot(window_len, buckets, farthest):
    exact_count = buckets // 2
    onehot = np.zeros((window_len, buckets), np.float32)
    for distance in range(window_len):
        if distance < exact_count:
            bucket = distance
        else:
            bucket = exact_count + int(math.log(distance / exact_count) / math.log(farthest / exact_count) * (buckets - exact_count))
        onehot[distance, min(bucket, buckets - 1)] = 1.0
    return onehot

def root_norm(values, gain_vec):
    return values * lax.rsqrt(lax.optimization_barrier(jnp.mean(values * values, axis=-1, keepdims=True)) + epsilon) * gain_vec

def dense_high(left_side, right_side):
    return jnp.dot(left_side, right_side, precision=highest)

def window_pass(weights, carried_in, inputs):
    w_query, w_key, w_value, w_out, w_state_out, w_up, w_down, state_query, init_state, gain_attn, gain_mlp, gain_state, state_gate, bias_table = weights
    carried, keys_prev, values_prev, flag_prev = carried_in
    window_x, window_starts, window_reset = inputs
    score_scale = 1.0 / math.sqrt(DH)
    normed = low(root_norm(window_x, gain_attn))
    queries = low(low_back(dense_high(normed, w_query))).reshape(W, H, DH)
    keys_cur = low(low_back(dense_high(normed, w_key))).reshape(W, H, DH)
    values_cur = low(low_back(dense_high(normed, w_value))).reshape(W, H, DH)
    segment = jnp.cumsum(window_starts)
    flag_cur = (segment == segment[-1]).astype(jnp.float32)
    state_queries = state_query.reshape(S, H, DH)
    state_logits = low_back(jnp.einsum('shd,khd->hsk', state_queries, keys_cur, precision=highest) * score_scale)
    state_probs = jax.nn.softmax(state_logits, axis=-1)
    state_mix = jnp.einsum('hsk,khd->shd', low(state_probs), values_cur, precision=highest).reshape(S, D)
    update = low_back(dense_high(low(low_back(state_mix)), w_state_out))
    state_normed = low(root_norm(carried, gain_state))
    keys_state = low(low_back(dense_high(state_normed, w_key))).reshape(S, H, DH)
    values_state = low(low_back(dense_high(state_normed, w_value))).reshape(S, H, DH)
    all_keys = jnp.concatenate([keys_prev, keys_cur, keys_state], axis=0)
    all_values = jnp.concatenate([values_prev, values_cur, values_state], axis=0)
    onehot = bucket_onehot(W, NB, MAXDIST)
    per_distance = dense_high(bias_table, jnp.asarray(onehot.T))
    rows_at = np.arange(W)[:, None]
    cols_at = np.arange(2 * W)[None, :]
    token_bias = per_distance[:, np.clip(rows_at + W - cols_at, 0, W - 1)]
    full_bias = jnp.concatenate([token_bias, jnp.zeros((H, W, S), jnp.float32)], axis=2)
    query_pos = jnp.arange(W)[:, None]
    key_pos = jnp.arange(W)[None, :]
    prev_ok = (key_pos > query_pos) & (segment[:, None] == 0) & (flag_prev[None, :] > 0.5)
    cur_ok = (key_pos <= query_pos) & (segment[:, None] == segment[None, :])
    allowed = jnp.concatenate([prev_ok, cur_ok, jnp.ones((W, S), jnp.bool_)], axis=1)
    logits = jnp.einsum('qhd,khd->hqk', queries, all_keys, precision=highest) * score_scale + full_bias
    logits = low_back(jnp.where(allowed[None], logits, -1e+30))
    softmax_probs = jax.nn.softmax(logits, axis=-1)
    mixture = jnp.einsum('hqk,khd->qhd', low(softmax_probs), all_values, precision=highest).reshape(W, D)
    branch = low_back(dense_high(low(low_back(mixture)), w_out))
    middle = window_x + branch
    hidden = low(root_norm(middle, gain_mlp))
    pre_act = low_back(dense_high(hidden, w_up))
    activation = low(jax.nn.gelu(pre_act, approximate=False))
    result = middle + low_back(dense_high(activation, w_down))
    decay_rate = state_gate * (1.0 - window_reset)
    offset = window_reset * init_state + (1.0 - window_reset) * (1.0 - state_gate) * update
    next_state = decay_rate * carried + offset
    return ((next_state, keys_cur, values_cur, flag_cur), result)

def reference(tokens, cotangent, doc_starts, state_resets, w_query, w_key, w_value, w_out, w_state_out, w_up, w_down, state_query, init_state, gain_attn, gain_mlp, gain_state, state_gate, bias_table):
    weights = tuple((weight_arg.astype(jnp.float32) for weight_arg in (w_query, w_key, w_value, w_out, w_state_out, w_up, w_down, state_query, init_state, gain_attn, gain_mlp, gain_state, state_gate, bias_table)))
    windows = STREAM // W
    seq_first = (jnp.arange(STREAM) % SEQ == 0)[None, :]
    starts = jnp.where(seq_first, 1, doc_starts).astype(jnp.int32)
    seq_last = ((jnp.arange(windows) + 1) % SEQ_WIN == 0)[None, :]
    resets = jnp.where(seq_last, 1, state_resets).astype(jnp.float32)
    window_step = jax.checkpoint(window_pass)

    def forward(weight_set, inputs):

        def one_stream(stream):
            stream_x, stream_starts, stream_resets = stream
            initial = (weight_set[8], jnp.zeros((W, H, DH), jnp.float32), jnp.zeros((W, H, DH), jnp.float32), jnp.zeros((W,), jnp.float32))

            def advance(carried_in, window_in):
                return window_step(weight_set, carried_in, window_in)
            last_carry, outputs = lax.scan(advance, initial, (stream_x.reshape(windows, W, D), stream_starts.reshape(windows, W), stream_resets))
            return outputs.reshape(STREAM, D)
        return lax.map(one_stream, (inputs, starts, resets))
    result, pull_back = jax.vjp(forward, weights, tokens.astype(jnp.float32))
    weight_grads, input_grad = pull_back(cotangent.astype(jnp.float32))
    return (result.astype(jnp.bfloat16), input_grad.astype(jnp.bfloat16), weight_grads[0], weight_grads[1], weight_grads[2], weight_grads[3], weight_grads[4], weight_grads[5], weight_grads[6], weight_grads[7], weight_grads[8], weight_grads[9], weight_grads[10], weight_grads[11], weight_grads[12], weight_grads[13])
```

```python
import functools
import math

import jax
import jax.numpy as jnp
import numpy as np
from jax import lax
from jax.experimental import pallas as pl
from jax.experimental.pallas import tpu as pltpu
from jax.sharding import PartitionSpec as P

H = 8
DH = 128
NB = 32
MAXDIST = 128
SEQ_WIN = 8


epsilon = 1e-06
highest = lax.Precision.HIGHEST


def shifted(shard, axis, by):
    devices = lax.axis_size(axis)
    pairs = [(i, i + by) for i in range(devices) if 0 <= i + by < devices]
    return lax.ppermute(shard, axis, pairs)


RELAY_ROWS = 32


def relay_kernel(step, chain_len, decay_ref, offset_ref, anchor_ref, out_ref, landed, leaving, send_sem, recv_sem):
    position = lax.axis_index("wide")
    place = lax.rem(position, SEQ_WIN)
    if step > 0:
        is_first = place == 0
        is_last = (place == SEQ_WIN - 1) | (position == chain_len - 1)
    else:
        is_first = (place == SEQ_WIN - 1) | (position == chain_len - 1)
        is_last = place == 0
    target = lax.rem(position + step + chain_len, chain_len)
    source = lax.rem(position - step + chain_len, chain_len)
    barrier = pltpu.get_barrier_semaphore()

    @pl.when(jnp.logical_not(is_first))
    def _():
        pl.semaphore_signal(barrier, inc=1, device_id={"wide": source}, device_id_type=pl.DeviceIdType.MESH)

    @pl.when(jnp.logical_not(is_last))
    def _():
        pl.semaphore_signal(barrier, inc=1, device_id={"wide": target}, device_id_type=pl.DeviceIdType.MESH)

    partners = jnp.where(is_first, 0, 1) + jnp.where(is_last, 0, 1)
    pl.semaphore_wait(barrier, partners)

    chunks = offset_ref.shape[0] // RELAY_ROWS
    decay = decay_ref[...]

    def copy_of(chunk):
        rows = pl.ds(pl.multiple_of(chunk * RELAY_ROWS, RELAY_ROWS), RELAY_ROWS)
        return pltpu.make_async_remote_copy(
            src_ref=leaving.at[rows],
            dst_ref=landed.at[rows],
            send_sem=send_sem.at[chunk],
            recv_sem=recv_sem.at[chunk],
            device_id={"wide": target},
            device_id_type=pl.DeviceIdType.MESH,
        )

    def one_chunk(chunk, state):
        rows = pl.ds(pl.multiple_of(chunk * RELAY_ROWS, RELAY_ROWS), RELAY_ROWS)

        @pl.when(is_first)
        def _():
            out_ref[rows, :] = anchor_ref[rows, :]

        @pl.when(jnp.logical_not(is_first))
        def _():
            copy_of(chunk).wait_recv()
            out_ref[rows, :] = landed[rows, :].astype(jnp.float32)

        @pl.when(jnp.logical_not(is_last))
        def _():
            leaving[rows, :] = (decay * out_ref[rows, :] + offset_ref[rows, :]).astype(jnp.bfloat16)
            copy_of(chunk).start()

        return state

    lax.fori_loop(0, chunks, one_chunk, 0)

    @pl.when(jnp.logical_not(is_last))
    def _():
        def finish(chunk, state):
            copy_of(chunk).wait_send()
            return state

        lax.fori_loop(0, chunks, finish, 0)


def relay(decay, offset, anchor, step, chain_len, collective):
    rows, columns = offset.shape
    vmem = pl.BlockSpec(memory_space=pltpu.VMEM)
    return pl.pallas_call(
        functools.partial(relay_kernel, step, chain_len),
        out_shape=jax.ShapeDtypeStruct((rows, columns), jnp.float32),
        in_specs=[vmem] * 3,
        out_specs=vmem,
        scratch_shapes=[
            pltpu.VMEM((rows, columns), jnp.bfloat16),
            pltpu.VMEM((rows, columns), jnp.bfloat16),
            pltpu.SemaphoreType.DMA((rows // RELAY_ROWS,)),
            pltpu.SemaphoreType.DMA((rows // RELAY_ROWS,)),
        ],
        compiler_params=pltpu.CompilerParams(collective_id=collective, has_side_effects=True),
        name="relay_forward" if step > 0 else "relay_backward",
    )(decay, offset, anchor)


def swap(shard, axis, bit):
    pairs = [(i, i ^ (1 << bit)) for i in range(lax.axis_size(axis))]
    return lax.ppermute(shard, axis, pairs)


def bits_of(count):
    assert count & (count - 1) == 0
    return count.bit_length() - 1


def my_bit(axis, bit):
    return lax.rem(lax.axis_index(axis) // (1 << bit), 2)


def halves(array, dim, mine):
    half = array.shape[dim] // 2
    keep = lax.dynamic_slice_in_dim(array, mine * half, half, dim)
    send = lax.dynamic_slice_in_dim(array, (1 - mine) * half, half, dim)
    return keep, send


def first_swap(product, right):
    mine = my_bit("batch", 0)
    keep, send = halves(right, 1, mine)
    arrived = swap(product(send).astype(jnp.bfloat16), "batch", 0)
    return (product(keep) + arrived.astype(jnp.float32)).astype(jnp.bfloat16)


def first_swap_of(array):
    mine = my_bit("batch", 0)
    keep, send = halves(array, 1, mine)
    arrived = swap(send.astype(jnp.bfloat16), "batch", 0)
    return (keep + arrived.astype(jnp.float32)).astype(jnp.bfloat16)


def orders(batch_bits, wide_bits):
    across = [("batch", bit) for bit in range(1, batch_bits)]
    along = [("wide", bit) for bit in range(1, wide_bits)]
    return across + along + [("wide", 0)], [("wide", 0)] + across + along


def sum_shares(partial, order):
    wide_bits = bits_of(lax.axis_size("wide"))
    batch_bits = bits_of(lax.axis_size("batch"))
    rows, columns = partial.shape
    array = partial.reshape((1 << wide_bits, rows >> wide_bits, columns))
    left = list(range(wide_bits))
    for axis, bit in order:
        mine = my_bit(axis, bit)
        if axis == "batch":
            keep, send = halves(array, 2, mine)
        else:
            place = left.index(bit)
            inner = 1 << place
            blocks = array.shape[0]
            split = array.reshape((blocks // (2 * inner), 2, inner) + array.shape[1:])
            keep = lax.dynamic_index_in_dim(split, mine, 1, keepdims=False)
            send = lax.dynamic_index_in_dim(split, 1 - mine, 1, keepdims=False)
            keep = keep.reshape((blocks // 2,) + array.shape[1:])
            send = send.reshape((blocks // 2,) + array.shape[1:])
            left.remove(bit)
        arrived = swap(send, axis, bit)
        array = (keep.astype(jnp.float32) + arrived.astype(jnp.float32)).astype(jnp.bfloat16)
    array = array[0]
    for bit in reversed(range(batch_bits)):
        other = swap(array, "batch", bit)
        mine = my_bit("batch", bit)
        array = jnp.concatenate(
            [jnp.where(mine == 0, array, other), jnp.where(mine == 0, other, array)], axis=1
        )
    return array


def sum_everywhere(array):
    for axis in ("batch", "wide"):
        for bit in range(bits_of(lax.axis_size(axis))):
            array = array + swap(array, axis, bit)
    return array


def bucket_onehot(window_len, buckets, farthest):
    exact_count = buckets // 2
    onehot = np.zeros((window_len, buckets), np.float32)
    for distance in range(window_len):
        if distance < exact_count:
            bucket = distance
        else:
            bucket = exact_count + int(
                math.log(distance / exact_count)
                / math.log(farthest / exact_count)
                * (buckets - exact_count)
            )
        onehot[distance, min(bucket, buckets - 1)] = 1.0
    return onehot


def root_norm(values, gain_vec):
    return (
        values * lax.rsqrt(jnp.mean(values * values, axis=-1, keepdims=True) + epsilon) * gain_vec
    )


def gelu_exact(values):
    return jax.nn.gelu(values, approximate=False)


def project(inputs, weight):
    return jnp.dot(inputs, weight, preferred_element_type=jnp.float32)


def project_back(gradient, weight):
    return jnp.einsum("re,de->rd", gradient, weight, preferred_element_type=jnp.float32)


def weight_grad(inputs, gradient):
    return jnp.einsum("rd,re->de", inputs, gradient, preferred_element_type=jnp.float32)


def distance_bias(bias_table, onehot, window_len):
    head_count = bias_table.shape[0]
    per_distance = jnp.dot(bias_table, jnp.asarray(onehot.T), precision=highest)
    row_full = jnp.concatenate(
        [
            jnp.zeros((head_count, 1), jnp.float32),
            per_distance[:, ::-1],
            jnp.zeros((head_count, window_len), jnp.float32),
        ],
        axis=1,
    )
    tiled_rows = jnp.tile(row_full, (1, window_len))[:, : 2 * window_len * window_len]
    return tiled_rows.reshape(head_count, window_len, 2 * window_len)


def distance_sums(region, window_len):
    head_count = region.shape[0]
    flattened = jnp.pad(
        region.reshape(head_count, 2 * window_len * window_len), ((0, 0), (0, window_len))
    )
    banded = flattened.reshape(head_count, window_len, 2 * window_len + 1)[:, :, 1 : window_len + 1]
    return jnp.sum(banded, axis=1)[:, ::-1]


def token_logits(queries, all_keys, full_bias, allowed, score_scale):
    logits = (
        jnp.einsum("bqhd,bkhd->bhqk", queries, all_keys, preferred_element_type=jnp.float32)
        * score_scale
        + full_bias[None]
    )
    return jnp.where(allowed[:, None], logits, -1e30)


def shards(
    tokens,
    cotangent,
    doc_starts,
    state_resets,
    w_query,
    w_key,
    w_value,
    w_out,
    w_state_out,
    w_up,
    w_down,
    state_query,
    init_state,
    gain_attn,
    gain_mlp,
    gain_state,
    state_gate,
    bias_table,
):
    streams, window_len, model_dim = tokens.shape
    state_count = state_query.shape[0]
    head_count = H
    head_size = DH
    score_scale = 1.0 / math.sqrt(head_size)
    position = lax.axis_index("wide")
    chain_len = lax.axis_size("wide")
    onehot = bucket_onehot(window_len, NB, MAXDIST)
    at_anchor = (jnp.arange(window_len)[None, :] == 0) & (position % SEQ_WIN == 0)
    starts = jnp.where(at_anchor, 1, doc_starts)
    segment = jnp.cumsum(starts, axis=1)
    flag_cur = (segment == segment[:, -1:]).astype(jnp.bfloat16)
    tokens_f32 = tokens.astype(jnp.float32)
    normed, attn_norm_back = jax.vjp(root_norm, tokens_f32, gain_attn)
    normed_low = normed.astype(jnp.bfloat16).reshape(streams * window_len, model_dim)
    head_shape = (streams, window_len, head_count, head_size)
    queries = project(normed_low, w_query).astype(jnp.bfloat16).reshape(head_shape)
    keys_cur = project(normed_low, w_key).astype(jnp.bfloat16).reshape(head_shape)
    values_cur = project(normed_low, w_value).astype(jnp.bfloat16).reshape(head_shape)
    keys_prev, values_prev, flag_prev = shifted((keys_cur, values_cur, flag_cur), "wide", 1)
    state_queries = state_query.reshape(state_count, head_count, head_size)
    state_logits = (
        jnp.einsum("shd,bkhd->bhsk", state_queries, keys_cur, preferred_element_type=jnp.float32)
        * score_scale
    )
    state_probs = jax.nn.softmax(state_logits, axis=-1)
    state_probs_low = state_probs.astype(jnp.bfloat16)
    state_mix = jnp.einsum(
        "bhsk,bkhd->bshd", state_probs_low, values_cur, preferred_element_type=jnp.float32
    )
    state_mix_low = state_mix.astype(jnp.bfloat16).reshape(streams * state_count, model_dim)
    update = project(state_mix_low, w_state_out).reshape(streams, state_count, model_dim)
    seq_last = (position + 1) % SEQ_WIN == 0
    reset_f32 = jnp.where(seq_last, 1, state_resets).astype(jnp.float32)[:, :, None]
    decay_rate = state_gate * (1.0 - reset_f32)
    offset = reset_f32 * init_state + (1.0 - reset_f32) * (1.0 - state_gate) * update
    carried = relay(decay_rate[0], offset[0], init_state, 1, chain_len, 0)[None]
    state_normed, state_norm_back = jax.vjp(root_norm, carried, gain_state)
    state_low = state_normed.astype(jnp.bfloat16).reshape(streams * state_count, model_dim)
    state_shape = (streams, state_count, head_count, head_size)
    keys_state = project(state_low, w_key).astype(jnp.bfloat16).reshape(state_shape)
    values_state = project(state_low, w_value).astype(jnp.bfloat16).reshape(state_shape)
    all_keys = jnp.concatenate([keys_prev, keys_cur, keys_state], axis=1)
    all_values = jnp.concatenate([values_prev, values_cur, values_state], axis=1)
    full_bias = jnp.concatenate(
        [
            distance_bias(bias_table, onehot, window_len),
            jnp.zeros((head_count, window_len, state_count), jnp.float32),
        ],
        axis=2,
    )
    query_pos = jnp.arange(window_len)[:, None]
    key_pos = jnp.arange(window_len)[None, :]
    prev_ok = (
        (key_pos > query_pos)[None] & (segment[:, :, None] == 0) & (flag_prev[:, None, :] > 0.5)
    )
    cur_ok = (key_pos <= query_pos)[None] & (segment[:, :, None] == segment[:, None, :])
    state_ok = jnp.ones((streams, window_len, state_count), jnp.bool_)
    allowed = jnp.concatenate([prev_ok, cur_ok, state_ok], axis=2)
    logits = token_logits(queries, all_keys, full_bias, allowed, score_scale)
    log_total = jax.nn.logsumexp(logits, axis=-1, keepdims=True)
    probs_low = jnp.exp(logits - log_total).astype(jnp.bfloat16)
    mixture = jnp.einsum(
        "bhqk,bkhd->bqhd", probs_low, all_values, preferred_element_type=jnp.float32
    )
    mixture_low = mixture.astype(jnp.bfloat16).reshape(streams * window_len, model_dim)
    branch = project(mixture_low, w_out).reshape(streams, window_len, model_dim)
    middle = tokens_f32 + branch
    hidden, mlp_norm_back = jax.vjp(root_norm, middle, gain_mlp)
    hidden_low = hidden.astype(jnp.bfloat16).reshape(streams * window_len, model_dim)
    pre_act = project(hidden_low, w_up)
    activation, gelu_back = jax.vjp(gelu_exact, pre_act)
    activation_low = activation.astype(jnp.bfloat16)
    result = middle + project(activation_low, w_down).reshape(streams, window_len, model_dim)
    output = result.astype(jnp.bfloat16)
    cot_f32 = cotangent.astype(jnp.float32)
    cot_rows = cotangent.reshape(streams * window_len, model_dim)
    order_a, order_b = orders(bits_of(lax.axis_size("batch")), bits_of(chain_len))
    share_down = sum_shares(
        first_swap(functools.partial(weight_grad, activation_low), cot_rows), order_b
    )
    (grad_pre,) = gelu_back(project_back(cot_rows, w_down))
    grad_pre_low = grad_pre.astype(jnp.bfloat16)
    share_up = sum_shares(
        first_swap(functools.partial(weight_grad, hidden_low), grad_pre_low), order_a
    )
    grad_hidden = project_back(grad_pre_low, w_up).reshape(streams, window_len, model_dim)
    middle_part, grad_gain_mlp = mlp_norm_back(grad_hidden)
    grad_middle = cot_f32 + middle_part
    grad_branch = grad_middle.astype(jnp.bfloat16).reshape(streams * window_len, model_dim)
    half_out = first_swap(functools.partial(weight_grad, mixture_low), grad_branch)
    grad_mix = project_back(grad_branch, w_out).astype(jnp.bfloat16).reshape(head_shape)
    probs_again = jnp.exp(
        token_logits(queries, all_keys, full_bias, allowed, score_scale) - log_total
    )
    grad_values_all = jnp.einsum(
        "bhqk,bqhd->bkhd",
        probs_again.astype(jnp.bfloat16),
        grad_mix,
        preferred_element_type=jnp.float32,
    )
    grad_probs = jnp.einsum(
        "bqhd,bkhd->bhqk", grad_mix, all_values, preferred_element_type=jnp.float32
    )
    grad_logits = probs_again * (
        grad_probs - jnp.sum(probs_again * grad_probs, axis=-1, keepdims=True)
    )
    grad_logits_low = grad_logits.astype(jnp.bfloat16)
    grad_queries = (
        jnp.einsum("bhqk,bkhd->bqhd", grad_logits_low, all_keys, preferred_element_type=jnp.float32)
        * score_scale
    )
    grad_keys_all = (
        jnp.einsum("bhqk,bqhd->bkhd", grad_logits_low, queries, preferred_element_type=jnp.float32)
        * score_scale
    )
    region = jnp.sum(grad_logits_low[:, :, :, : 2 * window_len].astype(jnp.float32), axis=0)
    grad_table = jnp.dot(distance_sums(region, window_len), jnp.asarray(onehot), precision=highest)
    grad_keys_prev = grad_keys_all[:, :window_len]
    grad_values_prev = grad_values_all[:, :window_len]
    grad_keys_next, grad_values_next = (
        shifted(grad_keys_prev.astype(jnp.bfloat16), "wide", -1).astype(grad_keys_prev.dtype),
        shifted(grad_values_prev.astype(jnp.bfloat16), "wide", -1).astype(grad_values_prev.dtype),
    )
    grad_keys_state = (
        grad_keys_all[:, 2 * window_len :]
        .astype(jnp.bfloat16)
        .reshape(streams * state_count, model_dim)
    )
    grad_values_state = (
        grad_values_all[:, 2 * window_len :]
        .astype(jnp.bfloat16)
        .reshape(streams * state_count, model_dim)
    )
    grad_state_normed = (
        project_back(grad_keys_state, w_key) + project_back(grad_values_state, w_value)
    ).reshape(streams, state_count, model_dim)
    grad_state_local, grad_gain_state = state_norm_back(grad_state_normed)

    after = relay(
        decay_rate[0], grad_state_local[0], jnp.zeros_like(init_state), -1, chain_len, 1
    )[None]
    total_here = grad_state_local + decay_rate * after
    grad_update = (
        ((1.0 - reset_f32) * (1.0 - state_gate) * after)
        .astype(jnp.bfloat16)
        .reshape(streams * state_count, model_dim)
    )
    half_state_out = first_swap(functools.partial(weight_grad, state_mix_low), grad_update)
    grad_state_mix = (
        project_back(grad_update, w_state_out).astype(jnp.bfloat16).reshape(state_shape)
    )
    grad_values_from_state = jnp.einsum(
        "bhsk,bshd->bkhd", state_probs_low, grad_state_mix, preferred_element_type=jnp.float32
    )
    grad_state_probs = jnp.einsum(
        "bshd,bkhd->bhsk", grad_state_mix, values_cur, preferred_element_type=jnp.float32
    )
    grad_state_logits = state_probs * (
        grad_state_probs - jnp.sum(state_probs * grad_state_probs, axis=-1, keepdims=True)
    )
    grad_state_logits_low = grad_state_logits.astype(jnp.bfloat16)
    grad_query_state = (
        jnp.einsum(
            "bhsk,bkhd->shd", grad_state_logits_low, keys_cur, preferred_element_type=jnp.float32
        )
        * score_scale
    )
    grad_keys_from_state = (
        jnp.einsum(
            "bhsk,shd->bkhd",
            grad_state_logits_low,
            state_queries,
            preferred_element_type=jnp.float32,
        )
        * score_scale
    )
    grad_gate = jnp.sum((1.0 - reset_f32) * after * (carried - update), axis=(0, 1))
    grad_init = jnp.sum(jnp.where(position % SEQ_WIN == 0, total_here, 0.0) + reset_f32 * after, axis=0)
    grad_keys_low = (
        (grad_keys_all[:, window_len : 2 * window_len] + grad_keys_next + grad_keys_from_state)
        .astype(jnp.bfloat16)
        .reshape(streams * window_len, model_dim)
    )
    grad_values_low = (
        (
            grad_values_all[:, window_len : 2 * window_len]
            + grad_values_next
            + grad_values_from_state
        )
        .astype(jnp.bfloat16)
        .reshape(streams * window_len, model_dim)
    )
    grad_queries_low = grad_queries.astype(jnp.bfloat16).reshape(streams * window_len, model_dim)
    half_query = first_swap(functools.partial(weight_grad, normed_low), grad_queries_low)
    both_low = jnp.concatenate([normed_low, state_low], axis=0)
    half_key = first_swap(
        functools.partial(weight_grad, both_low),
        jnp.concatenate([grad_keys_low, grad_keys_state], axis=0),
    )
    half_value = first_swap(
        functools.partial(weight_grad, both_low),
        jnp.concatenate([grad_values_low, grad_values_state], axis=0),
    )
    grad_normed = (
        project_back(grad_queries_low, w_query)
        + project_back(grad_keys_low, w_key)
        + project_back(grad_values_low, w_value)
    )
    tokens_part, grad_gain_attn = attn_norm_back(
        grad_normed.reshape(streams, window_len, model_dim)
    )
    tokens_grad = (grad_middle + tokens_part).astype(jnp.bfloat16)
    half_squery = first_swap_of(grad_query_state.reshape(state_count, model_dim))
    half_init = first_swap_of(grad_init)

    def joined(parts):
        return jnp.concatenate(
            [part.reshape(chain_len, part.shape[0] // chain_len, part.shape[1]) for part in parts],
            axis=1,
        ).reshape(-1, parts[0].shape[1])

    wide_rows, thin_rows = model_dim // chain_len, state_count // chain_len
    shares_a = sum_shares(joined([half_query, half_key, half_value]), order_a)
    shares_b = sum_shares(joined([half_out, half_state_out, half_squery, half_init]), order_b)
    share_query, share_key, share_value = jnp.split(shares_a.astype(jnp.float32), 3, axis=0)
    share_out, share_state_out, share_squery, share_init = jnp.split(
        shares_b.astype(jnp.float32),
        [wide_rows, 2 * wide_rows, 2 * wide_rows + thin_rows],
        axis=0,
    )
    share_up = share_up.astype(jnp.float32)
    share_down = share_down.astype(jnp.float32)
    small = jnp.concatenate(
        [
            jnp.stack([grad_gain_attn, grad_gain_mlp, grad_gain_state, grad_gate]).reshape(-1),
            grad_table.reshape(-1),
        ]
    ).reshape(-1, 128)
    small = jnp.pad(small, ((0, -small.shape[0] % 8), (0, 0)))
    flat = sum_everywhere(small).reshape(-1)
    total_gain_attn = flat[:model_dim]
    total_gain_mlp = flat[model_dim : 2 * model_dim]
    total_gain_state = flat[2 * model_dim : 3 * model_dim]
    total_gate = flat[3 * model_dim : 4 * model_dim]
    total_table = flat[4 * model_dim : 4 * model_dim + head_count * NB].reshape(head_count, NB)
    return (
        output,
        tokens_grad,
        share_query,
        share_key,
        share_value,
        share_out,
        share_state_out,
        share_up,
        share_down,
        share_squery,
        share_init,
        total_gain_attn,
        total_gain_mlp,
        total_gain_state,
        total_gate,
        total_table,
    )


def solution(mesh):
    placed = (
        P("batch", "wide", None),
        P("batch", "wide", None),
        P("batch", "wide"),
        P("batch", "wide"),
        P(),
        P(),
        P(),
        P(),
        P(),
        P(),
        P(),
        P(),
        P(),
        P(),
        P(),
        P(),
        P(),
        P(),
    )
    return jax.shard_map(
        shards,
        mesh=mesh,
        in_specs=placed,
        out_specs=(
            P("batch", "wide", None),
            P("batch", "wide", None),
            P("wide", None),
            P("wide", None),
            P("wide", None),
            P("wide", None),
            P("wide", None),
            P("wide", None),
            P("wide", None),
            P("wide", None),
            P("wide", None),
            P(),
            P(),
            P(),
            P(),
            P(),
        ),
        check_vma=False,
    )
```

```python
import functools
import math

import jax
import jax.numpy as jnp
import numpy as np
from jax import lax
from jax.experimental import pallas as pl
from jax.experimental.pallas import tpu as pltpu
from jax.sharding import PartitionSpec as P

H = 8
DH = 128
NB = 32
MAXDIST = 128
SEQ_WIN = 8


epsilon = 1e-06
highest = lax.Precision.HIGHEST


def shifted(shard, axis, by):
    devices = lax.axis_size(axis)
    pairs = [(i, i + by) for i in range(devices) if 0 <= i + by < devices]
    return lax.ppermute(shard, axis, pairs)


RELAY_ROWS = 32


def relay_kernel(step, chain_len, decay_ref, offset_ref, anchor_ref, out_ref, landed, leaving, send_sem, recv_sem):
    position = lax.axis_index("wide")
    place = lax.rem(position, SEQ_WIN)
    if step > 0:
        is_first = place == 0
        is_last = (place == SEQ_WIN - 1) | (position == chain_len - 1)
    else:
        is_first = (place == SEQ_WIN - 1) | (position == chain_len - 1)
        is_last = place == 0
    target = lax.rem(position + step + chain_len, chain_len)
    source = lax.rem(position - step + chain_len, chain_len)
    barrier = pltpu.get_barrier_semaphore()

    @pl.when(jnp.logical_not(is_first))
    def _():
        pl.semaphore_signal(barrier, inc=1, device_id={"wide": source}, device_id_type=pl.DeviceIdType.MESH)

    @pl.when(jnp.logical_not(is_last))
    def _():
        pl.semaphore_signal(barrier, inc=1, device_id={"wide": target}, device_id_type=pl.DeviceIdType.MESH)

    partners = jnp.where(is_first, 0, 1) + jnp.where(is_last, 0, 1)
    pl.semaphore_wait(barrier, partners)

    chunks = offset_ref.shape[0] // RELAY_ROWS
    decay = decay_ref[...]

    def copy_of(chunk):
        rows = pl.ds(pl.multiple_of(chunk * RELAY_ROWS, RELAY_ROWS), RELAY_ROWS)
        return pltpu.make_async_remote_copy(
            src_ref=leaving.at[rows],
            dst_ref=landed.at[rows],
            send_sem=send_sem.at[chunk],
            recv_sem=recv_sem.at[chunk],
            device_id={"wide": target},
            device_id_type=pl.DeviceIdType.MESH,
        )

    def one_chunk(chunk, state):
        rows = pl.ds(pl.multiple_of(chunk * RELAY_ROWS, RELAY_ROWS), RELAY_ROWS)

        @pl.when(is_first)
        def _():
            out_ref[rows, :] = anchor_ref[rows, :]

        @pl.when(jnp.logical_not(is_first))
        def _():
            copy_of(chunk).wait_recv()
            out_ref[rows, :] = landed[rows, :].astype(jnp.float32)

        @pl.when(jnp.logical_not(is_last))
        def _():
            leaving[rows, :] = (decay * out_ref[rows, :] + offset_ref[rows, :]).astype(jnp.bfloat16)
            copy_of(chunk).start()

        return state

    lax.fori_loop(0, chunks, one_chunk, 0)

    @pl.when(jnp.logical_not(is_last))
    def _():
        def finish(chunk, state):
            copy_of(chunk).wait_send()
            return state

        lax.fori_loop(0, chunks, finish, 0)


def relay(decay, offset, anchor, step, chain_len, collective):
    rows, columns = offset.shape
    vmem = pl.BlockSpec(memory_space=pltpu.VMEM)
    return pl.pallas_call(
        functools.partial(relay_kernel, step, chain_len),
        out_shape=jax.ShapeDtypeStruct((rows, columns), jnp.float32),
        in_specs=[vmem] * 3,
        out_specs=vmem,
        scratch_shapes=[
            pltpu.VMEM((rows, columns), jnp.bfloat16),
            pltpu.VMEM((rows, columns), jnp.bfloat16),
            pltpu.SemaphoreType.DMA((rows // RELAY_ROWS,)),
            pltpu.SemaphoreType.DMA((rows // RELAY_ROWS,)),
        ],
        compiler_params=pltpu.CompilerParams(collective_id=collective, has_side_effects=True),
        name="relay_forward" if step > 0 else "relay_backward",
    )(decay, offset, anchor)


def swap(shard, axis, bit):
    pairs = [(i, i ^ (1 << bit)) for i in range(lax.axis_size(axis))]
    return lax.ppermute(shard, axis, pairs)


def bits_of(count):
    assert count & (count - 1) == 0
    return count.bit_length() - 1


def my_bit(axis, bit):
    return lax.rem(lax.axis_index(axis) // (1 << bit), 2)


def halves(array, dim, mine):
    half = array.shape[dim] // 2
    keep = lax.dynamic_slice_in_dim(array, mine * half, half, dim)
    send = lax.dynamic_slice_in_dim(array, (1 - mine) * half, half, dim)
    return keep, send


def first_swap(product, right):
    mine = my_bit("batch", 0)
    keep, send = halves(right, 1, mine)
    arrived = swap(product(send).astype(jnp.bfloat16), "batch", 0)
    return (product(keep) + arrived.astype(jnp.float32)).astype(jnp.bfloat16)


def first_swap_of(array):
    mine = my_bit("batch", 0)
    keep, send = halves(array, 1, mine)
    arrived = swap(send.astype(jnp.bfloat16), "batch", 0)
    return (keep + arrived.astype(jnp.float32)).astype(jnp.bfloat16)


def orders(batch_bits, wide_bits):
    across = [("batch", bit) for bit in range(1, batch_bits)]
    along = [("wide", bit) for bit in range(1, wide_bits)]
    return across + along + [("wide", 0)], [("wide", 0)] + across + along


def sum_shares(partial, order):
    wide_bits = bits_of(lax.axis_size("wide"))
    batch_bits = bits_of(lax.axis_size("batch"))
    rows, columns = partial.shape
    array = partial.reshape((1 << wide_bits, rows >> wide_bits, columns))
    left = list(range(wide_bits))
    for axis, bit in order:
        mine = my_bit(axis, bit)
        if axis == "batch":
            keep, send = halves(array, 2, mine)
        else:
            place = left.index(bit)
            inner = 1 << place
            blocks = array.shape[0]
            split = array.reshape((blocks // (2 * inner), 2, inner) + array.shape[1:])
            keep = lax.dynamic_index_in_dim(split, mine, 1, keepdims=False)
            send = lax.dynamic_index_in_dim(split, 1 - mine, 1, keepdims=False)
            keep = keep.reshape((blocks // 2,) + array.shape[1:])
            send = send.reshape((blocks // 2,) + array.shape[1:])
            left.remove(bit)
        arrived = swap(send, axis, bit)
        array = (keep.astype(jnp.float32) + arrived.astype(jnp.float32)).astype(jnp.bfloat16)
    array = array[0]
    for bit in reversed(range(batch_bits)):
        other = swap(array, "batch", bit)
        mine = my_bit("batch", bit)
        array = jnp.concatenate(
            [jnp.where(mine == 0, array, other), jnp.where(mine == 0, other, array)], axis=1
        )
    return array


def sum_everywhere(array):
    for axis in ("batch", "wide"):
        for bit in range(bits_of(lax.axis_size(axis))):
            array = array + swap(array, axis, bit)
    return array


def bucket_onehot(window_len, buckets, farthest):
    exact_count = buckets // 2
    onehot = np.zeros((window_len, buckets), np.float32)
    for distance in range(window_len):
        if distance < exact_count:
            bucket = distance
        else:
            bucket = exact_count + int(
                math.log(distance / exact_count)
                / math.log(farthest / exact_count)
                * (buckets - exact_count)
            )
        onehot[distance, min(bucket, buckets - 1)] = 1.0
    return onehot


def root_norm(values, gain_vec):
    return (
        values * lax.rsqrt(jnp.mean(values * values, axis=-1, keepdims=True) + epsilon) * gain_vec
    )


def gelu_exact(values):
    return jax.nn.gelu(values, approximate=False)


def project(inputs, weight):
    return jnp.dot(inputs, weight, preferred_element_type=jnp.float32)


def project_back(gradient, weight):
    return jnp.einsum("re,de->rd", gradient, weight, preferred_element_type=jnp.float32)


def weight_grad(inputs, gradient):
    return jnp.einsum("rd,re->de", inputs, gradient, preferred_element_type=jnp.float32)


def dot_nt(left, right):
    return lax.dot_general(left, right, (((1,), (1,)), ((), ())), preferred_element_type=jnp.float32)


def dot_nn(left, right):
    return lax.dot_general(left, right, (((1,), (0,)), ((), ())), preferred_element_type=jnp.float32)


def dot_tn(left, right):
    return lax.dot_general(left, right, (((0,), (0,)), ((), ())), preferred_element_type=jnp.float32)


def circulant(base, rows):
    columns = base.shape[1]
    array = jnp.broadcast_to(base, (8, columns))
    row = lax.broadcasted_iota(jnp.int32, (8, columns), 0)
    for bit in (1, 2, 4):
        array = jnp.where((row & bit) != 0, pltpu.roll(array, bit, 1), array)
    while array.shape[0] < rows:
        array = jnp.concatenate([array, pltpu.roll(array, array.shape[0], 1)], axis=0)
    return array


def circulant_sums(array):
    columns = array.shape[1]
    while array.shape[0] > 8:
        half = array.shape[0] // 2
        array = array[:half] + pltpu.roll(array[half:], columns - half, 1)
    row = lax.broadcasted_iota(jnp.int32, (8, columns), 0)
    for bit in (4, 2, 1):
        array = jnp.where((row & bit) != 0, pltpu.roll(array, columns - bit, 1), array)
    return jnp.sum(array, axis=0, keepdims=True)


def mask_into(mask_ref, seg_row_ref, seg_col_ref, prev_col_ref):
    @pl.when(pl.program_id(0) == 0)
    def _():
        shape = mask_ref.shape
        is_cur = lax.broadcasted_iota(jnp.int32, shape, 0) <= lax.broadcasted_iota(jnp.int32, shape, 1)
        code = jnp.where(is_cur, seg_col_ref[...], prev_col_ref[...])
        mask_ref[...] = jnp.where(code == seg_row_ref[...], 0.0, -1e30)


def merged(place, turn, is_cur, of_cur, of_prev):
    if place < turn:
        return of_cur(place)
    if place > turn:
        return of_prev(place)
    return jnp.where(is_cur, of_cur(place), of_prev(place))


def attend_kernel(banded, scale, *refs):
    if banded:
        (q_ref, ks_ref, vs_ref, kp_ref, kc_ref, vp_ref, vc_ref, seg_row_ref, seg_col_ref, prev_col_ref, dist_ref,
         mix_ref, lse_ref, mask_ref) = refs
        mask_into(mask_ref, seg_row_ref, seg_col_ref, prev_col_ref)
    else:
        q_ref, ks_ref, vs_ref, mix_ref, lse_ref = refs
    count = q_ref.shape[0]
    block = count // 2
    at = [slice(turn * block, (turn + 1) * block) for turn in range(2)]
    if banded:
        bias = circulant(dist_ref[0], block)
        shape = (block, block)
        is_cur = lax.broadcasted_iota(jnp.int32, shape, 0) <= lax.broadcasted_iota(jnp.int32, shape, 1)
    for turn in range(2):
        q = q_ref[at[turn], :]
        logits = [dot_nt(ks_ref[...], q) * scale]
        if banded:
            for place in range(2):
                token = merged(
                    place,
                    turn,
                    is_cur,
                    lambda b: dot_nt(kc_ref[at[b], :], q),
                    lambda b: dot_nt(kp_ref[at[b], :], q),
                )
                logits.append(token * scale + bias[:, at[(turn - place) % 2]] + mask_ref[at[place], at[turn]])
        top = functools.reduce(jnp.maximum, [jnp.max(part, axis=0, keepdims=True) for part in logits])
        probs = [jnp.exp(part - top) for part in logits]
        total = sum(jnp.sum(part, axis=0, keepdims=True) for part in probs)
        mix = dot_tn(vs_ref[...], probs[0].astype(jnp.bfloat16))
        if banded:
            for place in range(2):
                part = probs[1 + place]
                if place <= turn:
                    seen = jnp.where(is_cur, part, 0.0) if place == turn else part
                    mix += dot_tn(vc_ref[at[place], :], seen.astype(jnp.bfloat16))
                if place >= turn:
                    seen = jnp.where(is_cur, 0.0, part) if place == turn else part
                    mix += dot_tn(vp_ref[at[place], :], seen.astype(jnp.bfloat16))
        mix_ref[at[turn], :] = jnp.transpose(mix * (1.0 / total)).astype(mix_ref.dtype)
        lse_ref[0, :, at[turn]] = top + jnp.log(total)


def attend_back_kernel(banded, scale, *refs):
    if banded:
        (q_ref, ks_ref, vs_ref, grad_ref, lse_ref, kp_ref, kc_ref, vp_ref, vc_ref, seg_row_ref, seg_col_ref,
         prev_col_ref, dist_ref, gq_ref, gks_ref, gvs_ref, gkp_ref, gkc_ref, gvp_ref, gvc_ref, gdist_ref,
         mask_ref) = refs
        mask_into(mask_ref, seg_row_ref, seg_col_ref, prev_col_ref)
    else:
        q_ref, ks_ref, vs_ref, grad_ref, lse_ref, gq_ref, gks_ref, gvs_ref = refs
    count = q_ref.shape[0]
    block = count // 2
    at = [slice(turn * block, (turn + 1) * block) for turn in range(2)]
    if banded:
        bias = circulant(dist_ref[0], block)
        shape = (block, block)
        is_cur = lax.broadcasted_iota(jnp.int32, shape, 0) <= lax.broadcasted_iota(jnp.int32, shape, 1)
    sums = {}

    def add(name, value):
        sums[name] = sums[name] + value if name in sums else value

    for turn in range(2):
        q = q_ref[at[turn], :]
        grad = grad_ref[at[turn], :]
        lse = lse_ref[0, :, at[turn]]
        probs = [jnp.exp(dot_nt(ks_ref[...], q) * scale - lse)]
        grad_probs = [dot_nt(vs_ref[...], grad)]
        if banded:
            for place in range(2):
                token = merged(
                    place,
                    turn,
                    is_cur,
                    lambda b: dot_nt(kc_ref[at[b], :], q),
                    lambda b: dot_nt(kp_ref[at[b], :], q),
                )
                shift = bias[:, at[(turn - place) % 2]] + mask_ref[at[place], at[turn]]
                probs.append(jnp.exp(token * scale + shift - lse))
                grad_probs.append(
                    merged(
                        place,
                        turn,
                        is_cur,
                        lambda b: dot_nt(vc_ref[at[b], :], grad),
                        lambda b: dot_nt(vp_ref[at[b], :], grad),
                    )
                )
        delta = sum(jnp.sum(p * g, axis=0, keepdims=True) for p, g in zip(probs, grad_probs))
        grads = [p * (g - delta) for p, g in zip(probs, grad_probs)]
        low = grads[0].astype(jnp.bfloat16)
        add("vs", dot_nn(probs[0].astype(jnp.bfloat16), grad))
        add("ks", dot_nn(low, q))
        gq = dot_tn(ks_ref[...], low)
        if banded:
            for place in range(2):
                p, g = probs[1 + place], grads[1 + place]
                add(("d", (turn - place) % 2), g)
                if place <= turn:
                    pc = jnp.where(is_cur, p, 0.0) if place == turn else p
                    gc = jnp.where(is_cur, g, 0.0) if place == turn else g
                    gc = gc.astype(jnp.bfloat16)
                    add(("vc", place), dot_nn(pc.astype(jnp.bfloat16), grad))
                    add(("kc", place), dot_nn(gc, q))
                    gq += dot_tn(kc_ref[at[place], :], gc)
                if place >= turn:
                    pp = jnp.where(is_cur, 0.0, p) if place == turn else p
                    gp = jnp.where(is_cur, 0.0, g) if place == turn else g
                    gp = gp.astype(jnp.bfloat16)
                    add(("vp", place), dot_nn(pp.astype(jnp.bfloat16), grad))
                    add(("kp", place), dot_nn(gp, q))
                    gq += dot_tn(kp_ref[at[place], :], gp)
        gq_ref[at[turn], :] = (jnp.transpose(gq) * scale).astype(gq_ref.dtype)
    gks_ref[...] = (sums["ks"] * scale).astype(gks_ref.dtype)
    gvs_ref[...] = sums["vs"].astype(gvs_ref.dtype)
    if banded:
        for place in range(2):
            gkp_ref[at[place], :] = (sums["kp", place] * scale).astype(gkp_ref.dtype)
            gkc_ref[at[place], :] = (sums["kc", place] * scale).astype(gkc_ref.dtype)
            gvp_ref[at[place], :] = sums["vp", place].astype(gvp_ref.dtype)
            gvc_ref[at[place], :] = sums["vc", place].astype(gvc_ref.dtype)
        gdist_ref[0] = circulant_sums(jnp.concatenate([sums["d", 0], sums["d", 1]], axis=1))


def head_block(array):
    return pl.BlockSpec((array.shape[0], DH), lambda head: (0, head))


def whole_block(array):
    return pl.BlockSpec(array.shape, lambda head: (0,) * array.ndim)


def row_block(columns):
    return pl.BlockSpec((1, 1, columns), lambda head: (head, 0, 0))


def attend(q, ks, vs, band, name):
    count, columns = q.shape
    heads = columns // DH
    operands, specs, scratch = [q, ks, vs], [head_block(a) for a in (q, ks, vs)], []
    if band is not None:
        operands += band
        specs += [head_block(a) for a in band[:4]] + [whole_block(a) for a in band[4:7]] + [row_block(count)]
        scratch = [pltpu.VMEM((count, count), jnp.float32)]
    rows = ks.shape[0] * (1 if band is None else 2)
    return pl.pallas_call(
        functools.partial(attend_kernel, band is not None, 1.0 / math.sqrt(DH)),
        grid=(heads,),
        out_shape=(
            jax.ShapeDtypeStruct((count, columns), jnp.bfloat16),
            jax.ShapeDtypeStruct((heads, 1, count), jnp.float32),
        ),
        in_specs=specs,
        out_specs=(head_block(q), row_block(count)),
        scratch_shapes=scratch,
        cost_estimate=pl.CostEstimate(
            flops=4 * count * rows * columns, bytes_accessed=16 * count * columns, transcendentals=heads * count * rows
        ),
        name=name,
    )(*operands)


def attend_back(q, ks, vs, grad, lse, band, kinds, name):
    count, columns = q.shape
    heads = columns // DH
    operands = [q, ks, vs, grad, lse]
    specs = [head_block(a) for a in (q, ks, vs, grad)] + [row_block(count)]
    outs = [jax.ShapeDtypeStruct(a.shape, kind) for a, kind in zip((q, ks, vs), kinds)]
    scratch = []
    if band is not None:
        operands += band
        specs += [head_block(a) for a in band[:4]] + [whole_block(a) for a in band[4:7]] + [row_block(count)]
        outs += [jax.ShapeDtypeStruct(a.shape, kind) for a, kind in zip(band[:4], kinds[3:])]
        scratch = [pltpu.VMEM((count, count), jnp.float32)]
    out_specs = [head_block(a) for a in outs]
    if band is not None:
        outs.append(jax.ShapeDtypeStruct((heads, 1, count), jnp.float32))
        out_specs.append(row_block(count))
    rows = ks.shape[0] * (1 if band is None else 2)
    return pl.pallas_call(
        functools.partial(attend_back_kernel, band is not None, 1.0 / math.sqrt(DH)),
        grid=(heads,),
        out_shape=tuple(outs),
        in_specs=specs,
        out_specs=tuple(out_specs),
        scratch_shapes=scratch,
        cost_estimate=pl.CostEstimate(
            flops=10 * count * rows * columns, bytes_accessed=32 * count * columns, transcendentals=heads * count * rows
        ),
        name=name,
    )(*operands)


def shards(
    tokens,
    cotangent,
    doc_starts,
    state_resets,
    w_query,
    w_key,
    w_value,
    w_out,
    w_state_out,
    w_up,
    w_down,
    state_query,
    init_state,
    gain_attn,
    gain_mlp,
    gain_state,
    state_gate,
    bias_table,
):
    streams, window_len, model_dim = tokens.shape
    state_count = state_query.shape[0]
    head_count = H
    position = lax.axis_index("wide")
    chain_len = lax.axis_size("wide")
    onehot = bucket_onehot(window_len, NB, MAXDIST)
    at_anchor = (jnp.arange(window_len)[None, :] == 0) & (position % SEQ_WIN == 0)
    starts = jnp.where(at_anchor, 1, doc_starts)
    segment = jnp.cumsum(starts, axis=1)
    flag_cur = (segment == segment[:, -1:]).astype(jnp.bfloat16)
    tokens_f32 = tokens.astype(jnp.float32)
    normed, attn_norm_back = jax.vjp(root_norm, tokens_f32, gain_attn)
    normed_low = normed.astype(jnp.bfloat16).reshape(streams * window_len, model_dim)
    queries = project(normed_low, w_query).astype(jnp.bfloat16)
    keys_cur = project(normed_low, w_key).astype(jnp.bfloat16)
    values_cur = project(normed_low, w_value).astype(jnp.bfloat16)
    keys_prev, values_prev, flag_prev = shifted((keys_cur, values_cur, flag_cur), "wide", 1)
    state_mix_low, state_lse = attend(state_query, keys_cur, values_cur, None, "state_attend")
    update = project(state_mix_low, w_state_out).reshape(streams, state_count, model_dim)
    seq_last = (position + 1) % SEQ_WIN == 0
    reset_f32 = jnp.where(seq_last, 1, state_resets).astype(jnp.float32)[:, :, None]
    decay_rate = state_gate * (1.0 - reset_f32)
    offset = reset_f32 * init_state + (1.0 - reset_f32) * (1.0 - state_gate) * update
    carried = relay(decay_rate[0], offset[0], init_state, 1, chain_len, 0)[None]
    state_normed, state_norm_back = jax.vjp(root_norm, carried, gain_state)
    state_low = state_normed.astype(jnp.bfloat16).reshape(streams * state_count, model_dim)
    keys_state = project(state_low, w_key).astype(jnp.bfloat16)
    values_state = project(state_low, w_value).astype(jnp.bfloat16)
    per_distance = jnp.dot(bias_table, jnp.asarray(onehot.T), precision=highest)
    band = [
        keys_prev,
        keys_cur,
        values_prev,
        values_cur,
        segment.reshape(1, window_len),
        segment.reshape(window_len, 1),
        jnp.where(flag_prev > 0.5, 0, -1).reshape(window_len, 1),
        per_distance.reshape(head_count, 1, window_len),
    ]
    mixture_low, log_total = attend(queries, keys_state, values_state, band, "attend")
    branch = project(mixture_low, w_out).reshape(streams, window_len, model_dim)
    middle = tokens_f32 + branch
    hidden, mlp_norm_back = jax.vjp(root_norm, middle, gain_mlp)
    hidden_low = hidden.astype(jnp.bfloat16).reshape(streams * window_len, model_dim)
    pre_act = project(hidden_low, w_up)
    activation, gelu_back = jax.vjp(gelu_exact, pre_act)
    activation_low = activation.astype(jnp.bfloat16)
    result = middle + project(activation_low, w_down).reshape(streams, window_len, model_dim)
    output = result.astype(jnp.bfloat16)
    cot_f32 = cotangent.astype(jnp.float32)
    cot_rows = cotangent.reshape(streams * window_len, model_dim)
    order_a, order_b = orders(bits_of(lax.axis_size("batch")), bits_of(chain_len))
    share_down = sum_shares(
        first_swap(functools.partial(weight_grad, activation_low), cot_rows), order_b
    )
    (grad_pre,) = gelu_back(project_back(cot_rows, w_down))
    grad_pre_low = grad_pre.astype(jnp.bfloat16)
    share_up = sum_shares(
        first_swap(functools.partial(weight_grad, hidden_low), grad_pre_low), order_a
    )
    grad_hidden = project_back(grad_pre_low, w_up).reshape(streams, window_len, model_dim)
    middle_part, grad_gain_mlp = mlp_norm_back(grad_hidden)
    grad_middle = cot_f32 + middle_part
    grad_branch = grad_middle.astype(jnp.bfloat16).reshape(streams * window_len, model_dim)
    half_out = first_swap(functools.partial(weight_grad, mixture_low), grad_branch)
    grad_mix = project_back(grad_branch, w_out).astype(jnp.bfloat16)
    low, full = jnp.bfloat16, jnp.float32
    (
        grad_queries_low,
        grad_keys_state,
        grad_values_state,
        grad_keys_prev,
        grad_keys_here,
        grad_values_prev,
        grad_values_here,
        by_distance,
    ) = attend_back(
        queries,
        keys_state,
        values_state,
        grad_mix,
        log_total,
        band,
        (low, low, low, low, full, low, full),
        "attend_back",
    )
    grad_table = jnp.dot(
        by_distance.reshape(head_count, window_len), jnp.asarray(onehot), precision=highest
    )
    grad_keys_next, grad_values_next = shifted((grad_keys_prev, grad_values_prev), "wide", -1)
    grad_state_normed = (
        project_back(grad_keys_state, w_key) + project_back(grad_values_state, w_value)
    ).reshape(streams, state_count, model_dim)
    grad_state_local, grad_gain_state = state_norm_back(grad_state_normed)

    after = relay(
        decay_rate[0], grad_state_local[0], jnp.zeros_like(init_state), -1, chain_len, 1
    )[None]
    total_here = grad_state_local + decay_rate * after
    grad_update = (
        ((1.0 - reset_f32) * (1.0 - state_gate) * after)
        .astype(jnp.bfloat16)
        .reshape(streams * state_count, model_dim)
    )
    half_state_out = first_swap(functools.partial(weight_grad, state_mix_low), grad_update)
    grad_state_mix = project_back(grad_update, w_state_out).astype(jnp.bfloat16)
    grad_query_state, grad_keys_from_state, grad_values_from_state = attend_back(
        state_query,
        keys_cur,
        values_cur,
        grad_state_mix,
        state_lse,
        None,
        (full, full, full),
        "state_attend_back",
    )
    grad_gate = jnp.sum((1.0 - reset_f32) * after * (carried - update), axis=(0, 1))
    grad_init = jnp.sum(jnp.where(position % SEQ_WIN == 0, total_here, 0.0) + reset_f32 * after, axis=0)
    grad_keys_low = (
        grad_keys_here + grad_keys_next.astype(jnp.float32) + grad_keys_from_state
    ).astype(jnp.bfloat16)
    grad_values_low = (
        grad_values_here + grad_values_next.astype(jnp.float32) + grad_values_from_state
    ).astype(jnp.bfloat16)
    half_query = first_swap(functools.partial(weight_grad, normed_low), grad_queries_low)
    both_low = jnp.concatenate([normed_low, state_low], axis=0)
    half_key = first_swap(
        functools.partial(weight_grad, both_low),
        jnp.concatenate([grad_keys_low, grad_keys_state], axis=0),
    )
    half_value = first_swap(
        functools.partial(weight_grad, both_low),
        jnp.concatenate([grad_values_low, grad_values_state], axis=0),
    )
    grad_normed = (
        project_back(grad_queries_low, w_query)
        + project_back(grad_keys_low, w_key)
        + project_back(grad_values_low, w_value)
    )
    tokens_part, grad_gain_attn = attn_norm_back(
        grad_normed.reshape(streams, window_len, model_dim)
    )
    tokens_grad = (grad_middle + tokens_part).astype(jnp.bfloat16)
    half_squery = first_swap_of(grad_query_state)
    half_init = first_swap_of(grad_init)

    def joined(parts):
        return jnp.concatenate(
            [part.reshape(chain_len, part.shape[0] // chain_len, part.shape[1]) for part in parts],
            axis=1,
        ).reshape(-1, parts[0].shape[1])

    wide_rows, thin_rows = model_dim // chain_len, state_count // chain_len
    shares_a = sum_shares(joined([half_query, half_key, half_value]), order_a)
    shares_b = sum_shares(joined([half_out, half_state_out, half_squery, half_init]), order_b)
    share_query, share_key, share_value = jnp.split(shares_a.astype(jnp.float32), 3, axis=0)
    share_out, share_state_out, share_squery, share_init = jnp.split(
        shares_b.astype(jnp.float32),
        [wide_rows, 2 * wide_rows, 2 * wide_rows + thin_rows],
        axis=0,
    )
    share_up = share_up.astype(jnp.float32)
    share_down = share_down.astype(jnp.float32)
    small = jnp.concatenate(
        [
            jnp.stack([grad_gain_attn, grad_gain_mlp, grad_gain_state, grad_gate]).reshape(-1),
            grad_table.reshape(-1),
        ]
    ).reshape(-1, 128)
    small = jnp.pad(small, ((0, -small.shape[0] % 8), (0, 0)))
    flat = sum_everywhere(small).reshape(-1)
    total_gain_attn = flat[:model_dim]
    total_gain_mlp = flat[model_dim : 2 * model_dim]
    total_gain_state = flat[2 * model_dim : 3 * model_dim]
    total_gate = flat[3 * model_dim : 4 * model_dim]
    total_table = flat[4 * model_dim : 4 * model_dim + head_count * NB].reshape(head_count, NB)
    return (
        output,
        tokens_grad,
        share_query,
        share_key,
        share_value,
        share_out,
        share_state_out,
        share_up,
        share_down,
        share_squery,
        share_init,
        total_gain_attn,
        total_gain_mlp,
        total_gain_state,
        total_gate,
        total_table,
    )


def solution(mesh):
    placed = (
        P("batch", "wide", None),
        P("batch", "wide", None),
        P("batch", "wide"),
        P("batch", "wide"),
        P(),
        P(),
        P(),
        P(),
        P(),
        P(),
        P(),
        P(),
        P(),
        P(),
        P(),
        P(),
        P(),
        P(),
    )
    return jax.shard_map(
        shards,
        mesh=mesh,
        in_specs=placed,
        out_specs=(
            P("batch", "wide", None),
            P("batch", "wide", None),
            P("wide", None),
            P("wide", None),
            P("wide", None),
            P("wide", None),
            P("wide", None),
            P("wide", None),
            P("wide", None),
            P("wide", None),
            P("wide", None),
            P(),
            P(),
            P(),
            P(),
            P(),
        ),
        check_vma=False,
    )
```
